32 devices in a mesh: row: 8 (over y, x, core), col: 4 (over z).
Axes of the slice: x: 2, y: 2, z: 4, core: 2. Of those that a mesh axis runs over, the one named last changes fastest.
Arguments:
- vectors_window: float32 [32, 8, 64, 1024], P(None, 'row', None, 'col'), may hold values from -6 to 6
- column_strip: float32 [32, 8, 64, 1024], P(None, 'row', None, 'col'), may hold values from -6 to 6
- row_strip: float32 [1024, 32, 4, 128], P('row', None, 'col'), may hold values from -6 to 6
- factor: float32 [1024, 1024], P('row', 'col'), may hold values from -2 to 2
- window_start: int32 [1], replicated, may hold values from 1 to 15360
- deflated: int32 [1], replicated, may hold values from 0 to 512
Outputs:
- vectors_updated: float32 [32, 8, 64, 1024], P(None, 'row', None, 'col')
- column_updated: float32 [32, 8, 64, 1024], P(None, 'row', None, 'col')
- row_updated: float32 [1024, 32, 4, 128], P('row', None, 'col')
The draws below stay inside these ranges and needn't reach their ends.
All inputs are finite; a program needn't handle non-finite values.
Results may differ from the reference program's by a relative error of at most 0.0003.
Values sent between devices are 32-bit elements; how exact they have to be, the bound alone decides.
A program may use at most 64 MiB of HBM per device.

```python
import math
import jax
import jax.numpy as jnp
from jax import lax

W = 1024
BLK = 64
CBLK = 128
ROUNDS = 32
N = 16384
CROUNDS = 32
N_ROW = 8
N_COL = 4


def draw_factor(key, part):
    noise_key, scale_key = jax.random.split(key)
    positions = jnp.arange(W, dtype=jnp.float32) / (W - 1)
    spread = jnp.exp(jax.random.uniform(scale_key, (W,), jnp.float32, -1.15, 1.15))
    entries = jnp.clip(jax.random.normal(noise_key, (W, W), jnp.float32), -5.0, 5.0)
    column_scale = spread * jnp.exp(0.5 * math.log(3.0) * positions) / 1.5
    return (entries * column_scale[None, :] / math.sqrt(W)).astype(jnp.float32)


def block_levels(rng, dims, cuts, smallest, top_value):
    def one(dim, parts):
        steps = jax.random.uniform(jax.random.fold_in(jax.random.fold_in(rng, 6), dim), (parts,), jnp.float32, smallest / len(cuts), top_value / len(cuts))
        return jnp.repeat(jnp.exp(steps), dims[dim] // parts).reshape((-1,) + (1,) * (len(dims) - dim - 1))

    gain = one(*cuts[0])
    for cut in cuts[1:]:
        gain = gain * one(*cut)
    return gain


def normal_values(rng, shape, scale, most, shards=(), kind=jnp.bfloat16):
    gain = block_levels(rng, shape, shards, -0.22, 0.18) if shards else 1.0
    result = jax.random.normal(rng, shape, jnp.float32) * scale * gain
    return jnp.minimum(jnp.maximum(result, -most), most).astype(kind)


def setup_inputs(seed: int = 0) -> dict:
    streams_of = jax.random.split(jax.random.key(seed), 7)
    vectors_window = normal_values(streams_of[0], (ROUNDS, N_ROW, BLK, W), 1.0, 6.0, ((1, 8), (3, 4)), jnp.float32)
    column_strip = normal_values(streams_of[1], (ROUNDS, N_ROW, BLK, W), 1.0, 6.0, ((1, 8), (3, 4)), jnp.float32)
    row_strip = normal_values(streams_of[2], (W, CROUNDS, N_COL, CBLK), 1.0, 6.0, ((0, 8), (2, 4)), jnp.float32)
    factor = draw_factor(jax.random.fold_in(streams_of[6], 71), 0)
    window_start = jax.random.randint(streams_of[4], (1,), 1, N - W + 1).astype(jnp.int32)
    deflated = jax.random.randint(streams_of[5], (1,), 0, W // 2 + 1).astype(jnp.int32)
    return dict(vectors_window=vectors_window, column_strip=column_strip, row_strip=row_strip, factor=factor, window_start=window_start, deflated=deflated)


def reflect(factor, deflated):
    columns = jnp.arange(W, dtype=jnp.int32)
    kept_count = W - deflated[0]
    spike_row = jnp.where(columns < kept_count, factor[0], 0.0)
    squares = jnp.sum(spike_row * spike_row)
    corner = factor[0, 0]
    magnitude = jnp.sqrt(squares + 1e-06)
    signum = jnp.where(corner >= 0, 1.0, -1.0)
    vector = spike_row + jnp.where(columns == 0, signum * magnitude, 0.0)
    denominator = squares + 2.0 * jnp.abs(corner) * magnitude + magnitude * magnitude
    scaling = 2.0 / denominator
    reflected_image = jnp.dot(factor, vector, precision=lax.Precision.HIGHEST)
    return factor - scaling * reflected_image[:, None] * vector[None, :]

def reference(vectors_window, column_strip, row_strip, factor, window_start, deflated):
    highest = lax.Precision.HIGHEST
    rotation = reflect(factor, deflated)
    start_row = window_start[0]
    z_matrix = vectors_window.reshape(N, W)
    vectors_updated = jnp.dot(z_matrix, rotation, precision=highest).reshape(vectors_window.shape)
    strip_matrix = column_strip.reshape(N, W)
    turned = jnp.dot(strip_matrix, rotation, precision=highest)
    row_number = jnp.arange(N, dtype=jnp.int32)
    column_updated = jnp.where(row_number[:, None] < start_row, turned, strip_matrix).reshape(column_strip.shape)
    row_panel = row_strip.reshape(W, N)
    rotated_rows = lax.dot_general(rotation, row_panel, (((0,), (0,)), ((), ())), precision=highest)
    column_number = jnp.arange(N, dtype=jnp.int32)
    row_updated = jnp.where(column_number[None, :] >= start_row + W, rotated_rows, row_panel).reshape(row_strip.shape)
    return (vectors_updated, column_updated, row_updated)
```

```python
import functools
import jax
import jax.numpy as jnp
from jax import lax
from jax.experimental import pallas as pl
from jax.experimental.pallas import tpu as pltpu
from jax.sharding import PartitionSpec as P

MESH = pl.DeviceIdType.MESH
ROUNDS_PER_CHUNK = 2
OWN_EARLY = 2
OWN_LEAD = 8
PASS_LEAD = 9
STRIP_FIRST = 6
PLACE_PIECES = 4


def drain(ref, sem):
    pltpu.make_async_copy(ref, ref, sem).wait()


def local(src, dst, sem):
    pltpu.make_async_copy(src, dst, sem).start()


def split(x):
    high = x.astype(jnp.bfloat16)
    low = (x - high.astype(jnp.float32)).astype(jnp.bfloat16)
    return high, low


def kernel(
    nr, nc, blk, s_chunks, r_first, zc, sc,
    start, deflated, z, s, r, f,
    zo, so, ro,
    fbuf, rot, rh, rl, th, tl,
    xb, xq, rv, rp, rr, rb, rq,
    load, f_far_send, f_own_recv, f_far_recv,
    f_row_send, f_row_recv, f_pass_send, f_pass_recv,
    x_send, x_own, x_far, o_send, o_recv, o_own, keep,
    r_in_send, r_in_recv, r_out_send, r_out_recv, r_own,
):
    row = lax.axis_index("row")
    col = lax.axis_index("col")
    tall, wide = f.shape
    width = nc * wide
    rows_per_chunk = z.shape[1]
    chunk_rounds = rows_per_chunk // blk
    chunks = zc + s_chunks
    crounds = r.shape[0] // tall
    lanes = r.shape[1]
    r_groups = crounds // nr
    half = nc // 2
    upper = col >= half
    base = jnp.where(upper, half, 0)
    far_base = half - base
    mid = jnp.where(upper, half, half - 1)
    far_mid = nc - 1 - mid
    mid_slot = jnp.where(upper, 0, half - 1)
    outer_base = jnp.where(upper, half + 1, 0)
    is_mid = col == mid
    sibling = row + 1 - 2 * lax.rem(row, 2)
    cores = nr // 2

    def send(src, dst, send_sem, recv_sem, target):
        pltpu.make_async_remote_copy(
            src_ref=src, dst_ref=dst, send_sem=send_sem, recv_sem=recv_sem,
            device_id=target, device_id_type=MESH,
        ).start()

    def row_peer(d):
        return lax.rem(row + d, nr)

    def half_peer(d):
        return base + lax.rem(col - base + d, half)

    local(f, fbuf.at[row, col], load.at[0])
    local(z, xb.at[pl.ds(0, zc), col], load.at[1])
    local(s, xb.at[pl.ds(zc, sc), col], load.at[2])
    local(r, rv, load.at[3])

    barrier = pltpu.get_barrier_semaphore()
    for d in range(1, nc):
        pl.semaphore_signal(
            barrier, inc=1, device_id={"col": lax.rem(col + d, nc)}, device_id_type=MESH
        )
    for d in range(1, nr):
        pl.semaphore_signal(barrier, inc=1, device_id={"row": row_peer(d)}, device_id_type=MESH)
    pl.semaphore_wait(barrier, nc + nr - 2)

    def own_chunk(k):
        @pl.when(is_mid)
        def _():
            send(xb.at[k, col], xb.at[k, col], x_send, x_far.at[k], {"col": far_mid})

        @pl.when(jnp.logical_not(is_mid))
        def _():
            send(xb.at[k, col], xb.at[k, col], x_send, x_own.at[k], {"col": mid})

    def pass_chunk(k):
        if half > 1:
            outers = pl.ds(outer_base, half - 1)
            drain(xb.at[k, pl.ds(0, half - 1)], x_own.at[k])
            send(xb.at[k, outers], xb.at[k, outers], x_send, x_far.at[k], {"col": far_mid})

    drain(fbuf.at[0, 0], load.at[0])

    @pl.when(is_mid)
    def _():
        send(fbuf.at[row, col], fbuf.at[row, col], f_far_send, f_far_recv, {"col": far_mid})

    for d in range(1, half):
        send(
            fbuf.at[row, col], fbuf.at[row, col], f_far_send, f_own_recv,
            {"col": half_peer(d)},
        )

    drain(xb.at[pl.ds(0, zc), 0], load.at[1])
    drain(xb.at[pl.ds(0, sc), 0], load.at[2])
    own_early = min(OWN_EARLY, chunks)
    own_first = min(max(OWN_LEAD, own_early), chunks)

    @pl.loop(0, jnp.where(is_mid, own_early, chunks))
    def _(k):
        own_chunk(k)

    drain(rv, load.at[3])
    if r_first < r_groups:
        @pl.loop(r_first * nr, crounds)
        def _(k):
            rp[k] = rv[pl.ds(k, tall, stride=crounds), :]

    def r_in():
        if r_first < r_groups:
            @pl.loop(r_first, r_groups)
            def _(g):
                for d in range(1, nr):
                    p = row_peer(d)
                    send(rp.at[g * nr + p], rb.at[g, row], r_in_send, r_in_recv.at[g], {"row": p})

    @pl.when(jnp.logical_not(is_mid))
    def _():
        r_in()

    if half > 1:
        drain(fbuf.at[0, pl.ds(0, half - 1)], f_own_recv)

        @pl.when(is_mid)
        def _():
            outers = pl.ds(outer_base, half - 1)
            send(
                fbuf.at[row, outers], fbuf.at[row, outers], f_far_send, f_far_recv,
                {"col": far_mid},
            )

    @pl.when(is_mid)
    def _():
        @pl.loop(own_early, own_first)
        def _(k):
            own_chunk(k)

    drain(fbuf.at[0, pl.ds(0, half)], f_far_recv)

    @pl.when(is_mid)
    def _():
        fars = pl.ds(far_base, half)
        for d in range(1, half):
            send(
                fbuf.at[row, fars], fbuf.at[row, fars], f_far_send, f_far_recv,
                {"col": half_peer(d)},
            )

    send(fbuf.at[row], fbuf.at[row], f_row_send, f_pass_recv.at[0], {"row": sibling})
    for d in range(1, cores):
        send(fbuf.at[row], fbuf.at[row], f_row_send, f_row_recv.at[d], {"row": row_peer(2 * d)})

    pass_first = min(PASS_LEAD, chunks)

    @pl.when(is_mid)
    def _():
        r_in()

        @pl.loop(0, pass_first)
        def _(k):
            pass_chunk(k)

            @pl.when(k + own_first < chunks)
            def _():
                own_chunk(k + own_first)

    for d in range(1, cores):
        drain(fbuf.at[0], f_row_recv.at[d])
        origin = row_peer(nr - 2 * d)
        send(fbuf.at[origin], fbuf.at[origin], f_pass_send, f_pass_recv.at[d], {"row": sibling})
    for d in range(cores):
        drain(fbuf.at[0], f_pass_recv.at[d])

    kept = width - deflated[0]
    squares = jnp.zeros((1, 1), jnp.float32)
    spikes = []
    for c in range(nc):
        lane = lax.broadcasted_iota(jnp.int32, (1, wide), 1) + c * wide
        part = jnp.where(lane < kept, fbuf[0, c, 0:1, :], 0.0)
        squares = squares + jnp.sum(part * part, axis=1, keepdims=True)
        spikes.append((lane, part))
    corner = fbuf[0, 0, 0:1, 0:1]
    magnitude = jnp.sqrt(squares + 1e-06)
    shift = jnp.where(corner >= 0, 1.0, -1.0) * magnitude
    scaling = 2.0 / (squares + 2.0 * jnp.abs(corner) * magnitude + magnitude * magnitude)
    vector = [part + jnp.where(lane == 0, shift, 0.0) for lane, part in spikes]

    @pl.loop(0, nr)
    def _(i):
        image = jnp.zeros((tall, 1), jnp.float32)
        for c in range(nc):
            image = image + jnp.sum(fbuf[i, c] * vector[c], axis=1, keepdims=True)
        image = image * scaling
        rows = pl.ds(pl.multiple_of(i * tall, tall), tall)
        for c in range(nc):
            rot[c, rows, :] = fbuf[i, c] - image * vector[c]

    @pl.when(is_mid)
    def _():
        @pl.loop(0, nr)
        def _(i):
            rows = pl.ds(pl.multiple_of(i * tall, tall), tall)
            for j in range(half):
                high, low = split(rot[base + j, rows, :])
                rh[rows, j * wide:(j + 1) * wide] = high
                rl[rows, j * wide:(j + 1) * wide] = low

    if r_first < r_groups:
        @pl.loop(0, width // 128)
        def _(i):
            rows = pl.ds(pl.multiple_of(i * 128, 128), 128)
            for c in range(nc):
                high, low = split(rot[c, rows, :].T)
                th[c * wide:(c + 1) * wide, rows] = high
                tl[c * wide:(c + 1) * wide, rows] = low

        def r_back(g):
            for d in range(1, nr):
                p = row_peer(d)
                send(
                    rq.at[g, p], rr.at[g * nr + row], r_out_send, r_out_recv, {"row": p}
                )

        def r_group(g):
            rb[g, row] = rp[g * nr + row]
            drain(rb.at[g, pl.ds(0, nr - 1)], r_in_recv.at[g])
            block = rb[g].reshape(width, lanes)
            high, low = split(block)
            pair = jnp.concatenate([high, low], axis=1)
            lane = lax.broadcasted_iota(jnp.int32, (1, lanes), 1)
            column = ((g * nr + row) * nc + col) * lanes + lane
            turned = column >= start[0] + width

            @pl.loop(0, nr)
            def _(q):
                rows = pl.ds(pl.multiple_of(q * tall, tall), tall)
                both = jnp.dot(th[rows, :], pair, preferred_element_type=jnp.float32)
                rest = jnp.dot(tl[rows, :], high, preferred_element_type=jnp.float32)
                total = both[:, :lanes] + both[:, lanes:] + rest
                rq[g, q] = jnp.where(turned, total, rb[g, q])

            rr[g * nr + row] = rq[g, row]

    if s_chunks < sc:
        local(
            xb.at[pl.ds(zc + s_chunks, sc - s_chunks), col],
            so.at[pl.ds(s_chunks, sc - s_chunks)], keep,
        )

    def give(k):
        def to(out, n):
            local(xq.at[k, mid_slot], out.at[n], o_own)
            for d in range(1, half):
                j = lax.rem(mid_slot + d, half)
                send(xq.at[k, j], out.at[n], o_send, o_recv, {"col": base + j})

        @pl.when(k < zc)
        def _():
            to(zo, k)

        if s_chunks:
            @pl.when(k >= zc)
            def _():
                to(so, k - zc)

    strip_groups = r_groups - r_first
    strip_first = min(STRIP_FIRST, chunks - 2 * strip_groups)

    @pl.loop(0, chunks)
    def _(k):
        @pl.when(is_mid)
        def _():
            @pl.when(k + pass_first < chunks)
            def _():
                pass_chunk(k + pass_first)

            @pl.when(k + pass_first + own_first < chunks)
            def _():
                own_chunk(k + pass_first + own_first)

            @pl.when(k > 0)
            def _():
                give(k - 1)

        if strip_groups > 0:
            step = k - strip_first
            g = r_first + step // 2

            @pl.when((step >= 0) & (step < 2 * strip_groups) & (lax.rem(step, 2) == 0))
            def _():
                r_group(g)

            @pl.when((step >= 0) & (step < 2 * strip_groups) & (lax.rem(step, 2) == 1))
            def _():
                r_back(g)

        @pl.when(is_mid)
        def _():
            drain(xb.at[k, pl.ds(0, half)], x_far.at[k])
            parts = [split(xb[k, c]) for c in range(nc)]
            high = jnp.concatenate([p[0] for p in parts], axis=1)
            low = jnp.concatenate([p[1] for p in parts], axis=1)
            both = jnp.dot(
                jnp.concatenate([high, low], axis=0), rh[...],
                preferred_element_type=jnp.float32,
            )
            total = both[:rows_per_chunk] + both[rows_per_chunk:]
            total = total + jnp.dot(high, rl[...], preferred_element_type=jnp.float32)
            index = lax.broadcasted_iota(jnp.int32, (rows_per_chunk, 1), 0)
            first = (k - zc) * chunk_rounds
            number = ((first + index // blk) * nr + row) * blk + lax.rem(index, blk)
            turned = number < jnp.where(k < zc, 2**30, start[0])
            for j in range(half):
                xq[k, j] = jnp.where(
                    turned, total[:, j * wide:(j + 1) * wide], xb[k, base + j]
                )

    @pl.when(is_mid)
    def _():
        give(chunks - 1)

    if r_first < r_groups:
        part = (r_groups - r_first) * (nr - 1)
        drain(rr.at[pl.ds(0, part)], r_out_recv)

        @pl.loop(r_first * nr, crounds)
        def _(k):
            rv[pl.ds(k, tall, stride=crounds), :] = rr[k]

    local(rv, ro, r_own)
    if r_first < r_groups:
        drain(rr.at[pl.ds(0, part)], r_out_send)
        drain(rr.at[pl.ds(0, part)], r_in_send)
    drain(fbuf.at[pl.ds(0, cores)], f_row_send)
    if cores > 1:
        drain(fbuf.at[pl.ds(0, cores - 1)], f_pass_send)
    if half > 1:
        drain(fbuf.at[0, pl.ds(0, half - 1)], f_far_send)

    @pl.when(is_mid)
    def _():
        drain(fbuf.at[0, pl.ds(0, half)], f_far_send)
        for d in range(1, half):
            drain(fbuf.at[0, pl.ds(0, half)], f_far_send)
        drain(xb.at[pl.ds(0, chunks), pl.ds(0, half)], x_send)
        if half > 1:
            drain(xq.at[pl.ds(0, chunks), pl.ds(0, half - 1)], o_send)
        drain(xq.at[pl.ds(0, chunks), 0], o_own)

    @pl.when(jnp.logical_not(is_mid))
    def _():
        drain(xb.at[pl.ds(0, chunks), 0], x_send)
        drain(xq.at[pl.ds(0, chunks), 0], o_recv)

    if s_chunks < sc:
        drain(so.at[pl.ds(s_chunks, sc - s_chunks)], keep)
    drain(rv, r_own)


def rotate(nr, nc, blk, s_chunks, r_first, ident, z, s, r, f, start, deflated):
    zc, rows_per_chunk, wide = z.shape
    sc = s.shape[0]
    tall = f.shape[0]
    width = nc * wide
    crounds = r.shape[0] // tall
    lanes = r.shape[1]
    r_groups = crounds // nr
    half = nc // 2
    chunks = zc + s_chunks
    smem = pl.BlockSpec(memory_space=pltpu.SMEM)
    hbm = pl.BlockSpec(memory_space=pltpu.HBM)
    f32 = jnp.float32
    bf16 = jnp.bfloat16
    dma = pltpu.SemaphoreType.DMA
    return pl.pallas_call(
        functools.partial(kernel, nr, nc, blk, s_chunks, r_first, zc, sc),
        out_shape=[jax.ShapeDtypeStruct(x.shape, f32) for x in (z, s, r)],
        in_specs=[smem] * 2 + [hbm] * 4,
        out_specs=[hbm] * 3,
        scratch_shapes=[
            pltpu.VMEM((nr, nc) + f.shape, f32),
            pltpu.VMEM((nc, width, wide), f32),
            pltpu.VMEM((width, half * wide), bf16),
            pltpu.VMEM((width, half * wide), bf16),
            pltpu.VMEM((width, width), bf16),
            pltpu.VMEM((width, width), bf16),
            pltpu.VMEM((zc + sc, nc, rows_per_chunk, wide), f32),
            pltpu.VMEM((chunks, half, rows_per_chunk, wide), f32),
            pltpu.VMEM(r.shape, f32),
            pltpu.VMEM((crounds, tall, lanes), f32),
            pltpu.VMEM((crounds, tall, lanes), f32),
            pltpu.VMEM((r_groups, nr, tall, lanes), f32),
            pltpu.VMEM((r_groups, nr, tall, lanes), f32),
            dma((4,)), dma, dma, dma,
            dma, dma((nr // 2,)), dma, dma((nr // 2,)),
            dma, dma((chunks,)), dma((chunks,)), dma, dma, dma, dma,
            dma, dma((r_groups,)), dma, dma, dma,
        ],
        compiler_params=pltpu.CompilerParams(
            collective_id=ident, has_side_effects=True, vmem_limit_bytes=52 * 1024 * 1024,
        ),
    )(start, deflated, z, s, r, f)


def place(z, s, r, zo, so, ro, sb, rb, out, inn):
    step = z.shape[0] // PLACE_PIECES
    for j in range(PLACE_PIECES):
        rows = pl.ds(j * step, step)
        local(s.at[rows], sb.at[rows], inn.at[0, j])
    strip_step = r.shape[0] // PLACE_PIECES
    for j in range(PLACE_PIECES):
        rows = pl.ds(j * strip_step, strip_step)
        local(r.at[rows], rb.at[rows], inn.at[1, j])
    local(z, zo, out.at[0])
    for i, size, src, dst in ((0, step, sb, so), (1, strip_step, rb, ro)):
        for j in range(PLACE_PIECES):
            rows = pl.ds(j * size, size)
            drain(src.at[rows], inn.at[i, j])
            local(src.at[rows], dst.at[rows], out.at[1 + i])
    drain(z, out.at[0])
    drain(sb, out.at[1])
    drain(rb, out.at[2])


def placed(z, s, r):
    hbm = pl.BlockSpec(memory_space=pltpu.HBM)
    return pl.pallas_call(
        place,
        out_shape=[jax.ShapeDtypeStruct(x.shape, x.dtype) for x in (z, s, r)],
        in_specs=[pl.BlockSpec(memory_space=pltpu.VMEM), hbm, hbm],
        out_specs=[hbm] * 3,
        scratch_shapes=[
            pltpu.VMEM(s.shape, s.dtype),
            pltpu.VMEM(r.shape, r.dtype),
            pltpu.SemaphoreType.DMA((3,)),
            pltpu.SemaphoreType.DMA((2, PLACE_PIECES)),
        ],
        compiler_params=pltpu.CompilerParams(vmem_limit_bytes=8 * 1024 * 1024),
    )(z, s, r)


def body(vectors_window, column_strip, row_strip, factor, window_start, deflated):
    nr = lax.axis_size("row")
    nc = lax.axis_size("col")
    rounds, _, blk, wide = vectors_window.shape
    tall, column_rounds, _, lanes = row_strip.shape
    width = nc * wide
    per = ROUNDS_PER_CHUNK
    z = vectors_window.reshape(rounds // per, per * blk, wide)
    s = column_strip.reshape(rounds // per, per * blk, wide)
    r = row_strip.reshape(tall * column_rounds, lanes)
    chunk_rows = per * blk * nr
    group_columns = lanes * nr * nc
    count = -(-(rounds * nr * blk - width) // chunk_rows)
    branches = [
        functools.partial(
            rotate, nr, nc, blk, k, ((k - 1) * chunk_rows + 1 + width) // group_columns, k - 1
        )
        for k in range(1, count + 1)
    ]
    choice = jnp.clip((window_start[0] - 1) // chunk_rows, 0, count - 1)
    zo, so, ro = lax.switch(choice, branches, z, s, r, factor, window_start, deflated)
    zo, so, ro = placed(zo, so, ro)
    return (
        zo.reshape(vectors_window.shape),
        so.reshape(column_strip.shape),
        ro.reshape(row_strip.shape),
    )


def solution(mesh):
    return jax.shard_map(
        body,
        mesh=mesh,
        in_specs=(
            P(None, "row", None, "col"),
            P(None, "row", None, "col"),
            P("row", None, "col", None),
            P("row", "col"),
            P(),
            P(),
        ),
        out_specs=(
            P(None, "row", None, "col"),
            P(None, "row", None, "col"),
            P("row", None, "col", None),
        ),
        check_vma=False,
    )
```

```python
import functools
import jax
import jax.numpy as jnp
from jax import lax
from jax.experimental import pallas as pl
from jax.experimental.pallas import tpu as pltpu
from jax.sharding import PartitionSpec as P

MESH = pl.DeviceIdType.MESH
ROUNDS_PER_CHUNK = 1
OWN_EARLY = 3
OWN_LEAD = 16
PASS_LEAD = 18
STRIP_FIRST = 12
STRIP_STEP = 3
OWNED = 2
COARSE = 6
TILE = 32
STRIP_EARLY = 2
PLACE_PIECES = 4


def drain(ref, sem):
    pltpu.make_async_copy(ref, ref, sem).wait()


def local(src, dst, sem):
    pltpu.make_async_copy(src, dst, sem).start()


def split(x):
    high = x.astype(jnp.bfloat16)
    low = (x - high.astype(jnp.float32)).astype(jnp.bfloat16)
    return high, low


def kernel(
    nr, nc, blk, s_chunks, r_first, zc, sc,
    start, deflated, z, s, r, f,
    zo, so, ro,
    fbuf, rot, rw, tw, acc, pair, xs,
    xb, xq, rv, rp, rr, rb, rq,
    load, f_far_send, f_own_recv, f_far_recv,
    f_row_send, f_row_recv, f_pass_send, f_pass_recv,
    x_send, x_own, x_far, o_send, o_recv, o_own, keep,
    r_in_send, r_in_recv, r_out_send, r_out_recv, r_own,
):
    row = lax.axis_index("row")
    col = lax.axis_index("col")
    tall, wide = f.shape
    width = nc * wide
    rows_per_chunk = z.shape[1]
    chunk_rounds = rows_per_chunk // blk
    chunks = zc + s_chunks
    crounds = r.shape[0] // tall
    lanes = r.shape[1]
    r_groups = crounds // nr
    half = nc // 2
    upper = col >= half
    base = jnp.where(upper, half, 0)
    far_base = half - base
    mid = jnp.where(upper, half, half - 1)
    far_mid = nc - 1 - mid
    mid_slot = jnp.where(upper, 0, half - 1)
    outer_base = jnp.where(upper, half + 1, 0)
    is_mid = col == mid
    sibling = row + 1 - 2 * lax.rem(row, 2)
    cores = nr // 2

    def send(src, dst, send_sem, recv_sem, target):
        pltpu.make_async_remote_copy(
            src_ref=src, dst_ref=dst, send_sem=send_sem, recv_sem=recv_sem,
            device_id=target, device_id_type=MESH,
        ).start()

    def row_peer(d):
        return lax.rem(row + d, nr)

    def half_peer(d):
        return base + lax.rem(col - base + d, half)

    local(f, fbuf.at[row, col], load.at[0])
    local(z, xb.at[pl.ds(0, zc), col], load.at[1])
    local(s, xb.at[pl.ds(zc, sc), col], load.at[2])
    local(r, rv, load.at[3])

    barrier = pltpu.get_barrier_semaphore()

    @pl.loop(1, nc)
    def _(d):
        pl.semaphore_signal(
            barrier, inc=1, device_id={"col": lax.rem(col + d, nc)}, device_id_type=MESH
        )

    @pl.loop(1, nr)
    def _(d):
        pl.semaphore_signal(barrier, inc=1, device_id={"row": row_peer(d)}, device_id_type=MESH)

    pl.semaphore_wait(barrier, nc + nr - 2)

    owned = min(OWNED, zc // 4)
    side = upper.astype(jnp.int32)

    def mine(k):
        return (k < 2 * owned) & (lax.rem(k, 2) == side)

    def theirs(k):
        return (k < 2 * owned) & (lax.rem(k, 2) != side)

    def own_chunk(k):
        @pl.when(is_mid & jnp.logical_not(mine(k)))
        def _():
            send(xb.at[k, col], xb.at[k, col], x_send, x_far.at[k], {"col": far_mid})

        @pl.when(jnp.logical_not(is_mid))
        def _():
            send(xb.at[k, col], xb.at[k, col], x_send, x_own.at[k], {"col": mid})

    def pass_chunk(k):
        if half > 1:
            outers = pl.ds(outer_base, half - 1)
            drain(xb.at[k, pl.ds(0, half - 1)], x_own.at[k])

            @pl.when(jnp.logical_not(mine(k)))
            def _():
                send(xb.at[k, outers], xb.at[k, outers], x_send, x_far.at[k], {"col": far_mid})

    drain(fbuf.at[0, 0], load.at[0])

    @pl.when(is_mid)
    def _():
        send(fbuf.at[row, col], fbuf.at[row, col], f_far_send, f_far_recv, {"col": far_mid})

    for d in range(1, half):
        send(
            fbuf.at[row, col], fbuf.at[row, col], f_far_send, f_own_recv,
            {"col": half_peer(d)},
        )

    drain(xb.at[pl.ds(0, zc), 0], load.at[1])
    drain(xb.at[pl.ds(0, sc), 0], load.at[2])
    own_early = min(OWN_EARLY, chunks)
    own_first = min(max(OWN_LEAD, own_early), chunks)

    @pl.loop(0, jnp.where(is_mid, own_early, chunks))
    def _(k):
        own_chunk(k)

    drain(rv, load.at[3])
    if r_first < r_groups:
        @pl.loop(r_first * nr, crounds)
        def _(k):
            @pl.loop(0, tall // TILE)
            def _(i):
                first = pl.multiple_of(i * TILE, TILE)
                rp[k, pl.ds(first, TILE), :] = rv[
                    pl.ds(k + first * crounds, TILE, stride=crounds), :
                ]

    def r_in(first, last):
        if r_first < r_groups:
            @pl.loop(first, last)
            def _(g):
                @pl.loop(1, nr)
                def _(d):
                    p = row_peer(d)
                    send(rp.at[g * nr + p], rb.at[g, row], r_in_send, r_in_recv.at[g], {"row": p})

    strip_early = min(r_first + STRIP_EARLY, r_groups)
    strip_split = jnp.where(is_mid, r_first, strip_early)
    r_in(r_first, strip_split)

    if half > 1:
        drain(fbuf.at[0, pl.ds(0, half - 1)], f_own_recv)

        @pl.when(is_mid)
        def _():
            outers = pl.ds(outer_base, half - 1)
            send(
                fbuf.at[row, outers], fbuf.at[row, outers], f_far_send, f_far_recv,
                {"col": far_mid},
            )

    @pl.when(is_mid)
    def _():
        @pl.loop(own_early, own_first)
        def _(k):
            own_chunk(k)

    drain(fbuf.at[0, pl.ds(0, half)], f_far_recv)

    @pl.when(is_mid)
    def _():
        fars = pl.ds(far_base, half)
        for d in range(1, half):
            send(
                fbuf.at[row, fars], fbuf.at[row, fars], f_far_send, f_far_recv,
                {"col": half_peer(d)},
            )

    send(fbuf.at[row], fbuf.at[row], f_row_send, f_pass_recv.at[0], {"row": sibling})

    @pl.loop(1, cores)
    def _(d):
        send(fbuf.at[row], fbuf.at[row], f_row_send, f_row_recv.at[d], {"row": row_peer(2 * d)})

    pass_first = min(PASS_LEAD, chunks)

    r_in(strip_split, r_groups)

    @pl.when(is_mid)
    def _():
        @pl.loop(0, pass_first)
        def _(k):
            pass_chunk(k)

            @pl.when(k + own_first < chunks)
            def _():
                own_chunk(k + own_first)

    @pl.loop(1, cores)
    def _(d):
        drain(fbuf.at[0], f_row_recv.at[d])
        origin = row_peer(nr - 2 * d)
        send(fbuf.at[origin], fbuf.at[origin], f_pass_send, f_pass_recv.at[d], {"row": sibling})

    @pl.loop(0, cores)
    def _(d):
        drain(fbuf.at[0], f_pass_recv.at[d])

    kept = width - deflated[0]
    squares = jnp.zeros((1, 1), jnp.float32)
    spikes = []
    for c in range(nc):
        lane = lax.broadcasted_iota(jnp.int32, (1, wide), 1) + c * wide
        part = jnp.where(lane < kept, fbuf[0, c, 0:1, :], 0.0)
        squares = squares + jnp.sum(part * part, axis=1, keepdims=True)
        spikes.append((lane, part))
    corner = fbuf[0, 0, 0:1, 0:1]
    magnitude = jnp.sqrt(squares + 1e-06)
    shift = jnp.where(corner >= 0, 1.0, -1.0) * magnitude
    scaling = 2.0 / (squares + 2.0 * jnp.abs(corner) * magnitude + magnitude * magnitude)
    vector = [part + jnp.where(lane == 0, shift, 0.0) for lane, part in spikes]

    tiles = tall // TILE

    @pl.loop(0, nr * tiles)
    def _(t):
        i = t // tiles
        inner = pl.ds(pl.multiple_of(lax.rem(t, tiles) * TILE, TILE), TILE)
        rows = pl.ds(pl.multiple_of(t * TILE, TILE), TILE)
        image = fbuf[i, 0, inner, :] * vector[0]
        for c in range(1, nc):
            image = image + fbuf[i, c, inner, :] * vector[c]
        image = jnp.sum(image, axis=1, keepdims=True) * scaling
        for c in range(nc):
            rot[c, rows, :] = fbuf[i, c, inner, :] - image * vector[c]

    @pl.when(is_mid)
    def _():
        @pl.loop(0, nr * tiles)
        def _(t):
            rows = pl.ds(pl.multiple_of(t * TILE, TILE), TILE)

            @pl.loop(0, nc)
            def _(j):
                high, low = split(rot[lax.rem(base + j, nc), rows, :])
                rw[2 * j, rows, :] = high
                rw[2 * j + 1, rows, :] = low

    if r_first < r_groups:
        @pl.loop(0, width // 128)
        def _(i):
            rows = pl.ds(pl.multiple_of(i * 128, 128), 128)

            @pl.loop(0, nc)
            def _(c):
                high, low = split(rot[c, rows, :].T)
                per = wide // tall
                for q in range(per):
                    piece = slice(q * tall, (q + 1) * tall)
                    tw[c * per + q, :tall, rows] = high[piece]
                    tw[c * per + q, tall:, rows] = low[piece]

        def r_back(g):
            @pl.loop(1, nr)
            def _(d):
                p = row_peer(d)
                send(
                    rq.at[g, p], rr.at[g * nr + row], r_out_send, r_out_recv, {"row": p}
                )

        def r_group(g):
            rb[g, row] = rp[g * nr + row]
            drain(rb.at[g, pl.ds(0, nr - 1)], r_in_recv.at[g])

            @pl.loop(0, nr)
            def _(q):
                rows = pl.ds(pl.multiple_of(q * tall, tall), tall)
                high, low = split(rb[g, q])
                pair[rows, :lanes] = high
                pair[rows, lanes:] = low

            lane = lax.broadcasted_iota(jnp.int32, (1, lanes), 1)
            column = ((g * nr + row) * nc + col) * lanes + lane
            turned = column >= start[0] + width

            @pl.loop(0, nr)
            def _(q):
                both = jnp.dot(tw[q], pair[...], preferred_element_type=jnp.float32)
                both = both[:tall] + both[tall:]
                total = both[:, :lanes] + both[:, lanes:]
                rq[g, q] = jnp.where(turned, total, rb[g, q])

            rr[g * nr + row] = rq[g, row]

        def r_place():
            drain(rr.at[pl.ds(0, (r_groups - r_first) * (nr - 1))], r_out_recv)

            @pl.loop(r_first * nr, crounds)
            def _(k):
                @pl.loop(0, tall // TILE)
                def _(i):
                    first = pl.multiple_of(i * TILE, TILE)
                    rv[pl.ds(k + first * crounds, TILE, stride=crounds), :] = rr[
                        k, pl.ds(first, TILE), :
                    ]

            local(rv, ro, r_own)

    if s_chunks < sc:
        local(
            xb.at[pl.ds(zc + s_chunks, sc - s_chunks), col],
            so.at[pl.ds(s_chunks, sc - s_chunks)], keep,
        )

    def give(k):
        def to(out, n):
            local(xq.at[k * half + mid_slot], out.at[n], o_own)
            for d in range(1, half):
                j = lax.rem(mid_slot + d, half)
                send(xq.at[k * half + j], out.at[n], o_send, o_recv, {"col": base + j})

        @pl.when((k < zc) & jnp.logical_not(theirs(k)))
        def _():
            to(zo, k)

        if s_chunks:
            @pl.when(k >= zc)
            def _():
                to(so, k - zc)

    def give_far():
        @pl.loop(0, owned)
        def _(n):
            @pl.loop(0, half)
            def _(j):
                send(
                    xq.at[(chunks + n) * half + j], zo.at[2 * n + side], o_send, o_recv,
                    {"col": far_base + j},
                )

    strip_groups = r_groups - r_first
    strip_span = STRIP_STEP * strip_groups
    strip_first = min(STRIP_FIRST, chunks - strip_span - 4)

    @pl.loop(0, chunks)
    def _(k):
        @pl.when(is_mid)
        def _():
            @pl.when(k + pass_first < chunks)
            def _():
                pass_chunk(k + pass_first)

            @pl.when(k + pass_first + own_first < chunks)
            def _():
                own_chunk(k + pass_first + own_first)

            @pl.when(k > 0)
            def _():
                give(k - 1)

            @pl.when(k == max(chunks - pass_first, 2 * owned + 1))
            def _():
                give_far()

        if strip_groups > 0:
            step = k - strip_first
            g = r_first + step // STRIP_STEP
            active = (step >= 0) & (step < strip_span)

            @pl.when(active & (lax.rem(step, STRIP_STEP) == 0))
            def _():
                r_group(g)

            @pl.when(active & (lax.rem(step, STRIP_STEP) == 1))
            def _():
                r_back(g)

            @pl.when(k == chunks - 4)
            def _():
                r_place()

        @pl.when(is_mid & jnp.logical_not(theirs(k)))
        def _():
            drain(xb.at[k, pl.ds(0, half)], x_far.at[k])

            @pl.loop(0, nc)
            def _(c):
                columns = pl.ds(pl.multiple_of(c * wide, wide), wide)
                high, low = split(xb[k, c])
                xs[:rows_per_chunk, columns] = high
                xs[rows_per_chunk:, columns] = low

            index = lax.broadcasted_iota(jnp.int32, (rows_per_chunk, 1), 0)
            first = (k - zc) * chunk_rounds
            number = ((first + index // blk) * nr + row) * blk + lax.rem(index, blk)
            turned = number < jnp.where(k < zc, 2**30, start[0])

            @pl.loop(0, jnp.where(mine(k), 2 * nc, 2 * half))
            def _(i):
                both = jnp.dot(xs[...], rw[i], preferred_element_type=jnp.float32)
                both = both[:rows_per_chunk] + both[rows_per_chunk:]

                @pl.when(lax.rem(i, 2) == 0)
                def _():
                    acc[...] = both

                @pl.when(lax.rem(i, 2) == 1)
                def _():
                    j = i // 2
                    slot = jnp.where(j < half, k, chunks + k // 2 - 1) * half + j
                    xq[slot] = jnp.where(
                        turned, acc[...] + both, xb[k, lax.rem(base + j, nc)]
                    )

    @pl.when(is_mid)
    def _():
        give(chunks - 1)

    if strip_groups > 0:
        part = strip_groups * (nr - 1)
        drain(rr.at[pl.ds(0, part)], r_out_send)
        drain(rr.at[pl.ds(0, part)], r_in_send)
    else:
        local(rv, ro, r_own)
    drain(fbuf.at[pl.ds(0, cores)], f_row_send)
    if cores > 1:
        drain(fbuf.at[pl.ds(0, cores - 1)], f_pass_send)
    if half > 1:
        drain(fbuf.at[0, pl.ds(0, half - 1)], f_far_send)

    @pl.when(is_mid)
    def _():
        drain(fbuf.at[0, pl.ds(0, half)], f_far_send)
        for d in range(1, half):
            drain(fbuf.at[0, pl.ds(0, half)], f_far_send)
        drain(xb.at[pl.ds(0, chunks - owned), pl.ds(0, half)], x_send)
        drain(xq.at[pl.ds(0, (chunks - owned) * (half - 1) + owned * half)], o_send)
        drain(xq.at[pl.ds(0, chunks - owned)], o_own)
        if owned:
            drain(xq.at[pl.ds(0, owned)], o_recv)

    @pl.when(jnp.logical_not(is_mid))
    def _():
        drain(xb.at[pl.ds(0, chunks), 0], x_send)
        drain(xq.at[pl.ds(0, chunks)], o_recv)

    if s_chunks < sc:
        drain(so.at[pl.ds(s_chunks, sc - s_chunks)], keep)
    drain(rv, r_own)


def rotate(nr, nc, blk, s_chunks, r_first, ident, z, s, r, f, start, deflated):
    zc, rows_per_chunk, wide = z.shape
    sc = s.shape[0]
    tall = f.shape[0]
    width = nc * wide
    crounds = r.shape[0] // tall
    lanes = r.shape[1]
    r_groups = crounds // nr
    half = nc // 2
    chunks = zc + s_chunks
    smem = pl.BlockSpec(memory_space=pltpu.SMEM)
    hbm = pl.BlockSpec(memory_space=pltpu.HBM)
    f32 = jnp.float32
    bf16 = jnp.bfloat16
    dma = pltpu.SemaphoreType.DMA
    return pl.pallas_call(
        functools.partial(kernel, nr, nc, blk, s_chunks, r_first, zc, sc),
        out_shape=[jax.ShapeDtypeStruct(x.shape, f32) for x in (z, s, r)],
        in_specs=[smem] * 2 + [hbm] * 4,
        out_specs=[hbm] * 3,
        scratch_shapes=[
            pltpu.VMEM((nr, nc) + f.shape, f32),
            pltpu.VMEM((nc, width, wide), f32),
            pltpu.VMEM((2 * nc, width, wide), bf16),
            pltpu.VMEM((nr, 2 * tall, width), bf16),
            pltpu.VMEM((rows_per_chunk, wide), f32),
            pltpu.VMEM((width, 2 * lanes), bf16),
            pltpu.VMEM((2 * rows_per_chunk, width), bf16),
            pltpu.VMEM((zc + sc, nc, rows_per_chunk, wide), f32),
            pltpu.VMEM(((chunks + min(OWNED, zc // 4)) * half, rows_per_chunk, wide), f32),
            pltpu.VMEM(r.shape, f32),
            pltpu.VMEM((crounds, tall, lanes), f32),
            pltpu.VMEM((crounds, tall, lanes), f32),
            pltpu.VMEM((r_groups, nr, tall, lanes), f32),
            pltpu.VMEM((r_groups, nr, tall, lanes), f32),
            dma((4,)), dma, dma, dma,
            dma, dma((nr // 2,)), dma, dma((nr // 2,)),
            dma, dma((chunks,)), dma((chunks,)), dma, dma, dma, dma,
            dma, dma((r_groups,)), dma, dma, dma,
        ],
        compiler_params=pltpu.CompilerParams(
            collective_id=ident, has_side_effects=True, vmem_limit_bytes=56 * 1024 * 1024,
        ),
    )(start, deflated, z, s, r, f)


def place(z, s, r, zo, so, ro, sb, rb, out, inn):
    step = z.shape[0] // PLACE_PIECES
    for j in range(PLACE_PIECES):
        rows = pl.ds(j * step, step)
        local(s.at[rows], sb.at[rows], inn.at[0, j])
    strip_step = r.shape[0] // PLACE_PIECES
    for j in range(PLACE_PIECES):
        rows = pl.ds(j * strip_step, strip_step)
        local(r.at[rows], rb.at[rows], inn.at[1, j])
    local(z, zo, out.at[0])
    for i, size, src, dst in ((0, step, sb, so), (1, strip_step, rb, ro)):
        for j in range(PLACE_PIECES):
            rows = pl.ds(j * size, size)
            drain(src.at[rows], inn.at[i, j])
            local(src.at[rows], dst.at[rows], out.at[1 + i])
    drain(z, out.at[0])
    drain(sb, out.at[1])
    drain(rb, out.at[2])


def placed(z, s, r):
    hbm = pl.BlockSpec(memory_space=pltpu.HBM)
    return pl.pallas_call(
        place,
        out_shape=[jax.ShapeDtypeStruct(x.shape, x.dtype) for x in (z, s, r)],
        in_specs=[pl.BlockSpec(memory_space=pltpu.VMEM), hbm, hbm],
        out_specs=[hbm] * 3,
        scratch_shapes=[
            pltpu.VMEM(s.shape, s.dtype),
            pltpu.VMEM(r.shape, r.dtype),
            pltpu.SemaphoreType.DMA((3,)),
            pltpu.SemaphoreType.DMA((2, PLACE_PIECES)),
        ],
        compiler_params=pltpu.CompilerParams(vmem_limit_bytes=8 * 1024 * 1024),
    )(z, s, r)


def body(vectors_window, column_strip, row_strip, factor, window_start, deflated):
    nr = lax.axis_size("row")
    nc = lax.axis_size("col")
    rounds, _, blk, wide = vectors_window.shape
    tall, column_rounds, _, lanes = row_strip.shape
    width = nc * wide
    per = ROUNDS_PER_CHUNK
    z = vectors_window.reshape(rounds // per, per * blk, wide)
    s = column_strip.reshape(rounds // per, per * blk, wide)
    r = row_strip.reshape(tall * column_rounds, lanes)
    chunk_rows = per * blk * nr
    group_columns = lanes * nr * nc
    count = -(-(rounds * nr * blk - width) // chunk_rows)
    coarse = COARSE if count > COARSE else 0
    sizes = [k for k in range(1, count + 1) if k > coarse or k % 2 == 0]
    bounds = [0] + sizes[:-1]
    branches = [
        functools.partial(
            rotate, nr, nc, blk, k, (low * chunk_rows + 1 + width) // group_columns, i
        )
        for i, (k, low) in enumerate(zip(sizes, bounds))
    ]
    last = jnp.clip((window_start[0] - 1) // chunk_rows, 0, count - 1)
    choice = jnp.where(last < coarse, last // 2, last - coarse // 2)
    zo, so, ro = lax.switch(choice, branches, z, s, r, factor, window_start, deflated)
    zo, so, ro = placed(zo, so, ro)
    return (
        zo.reshape(vectors_window.shape),
        so.reshape(column_strip.shape),
        ro.reshape(row_strip.shape),
    )


def solution(mesh):
    return jax.shard_map(
        body,
        mesh=mesh,
        in_specs=(
            P(None, "row", None, "col"),
            P(None, "row", None, "col"),
            P("row", None, "col", None),
            P("row", "col"),
            P(),
            P(),
        ),
        out_specs=(
            P(None, "row", None, "col"),
            P(None, "row", None, "col"),
            P("row", None, "col", None),
        ),
        check_vma=False,
    )
```

```python
import functools
import jax
import jax.numpy as jnp
from jax import lax
from jax.experimental import pallas as pl
from jax.experimental.pallas import tpu as pltpu
from jax.sharding import PartitionSpec as P

MESH = pl.DeviceIdType.MESH
ROUNDS_PER_CHUNK = 1
OWN_EARLY = 3
OWN_LEAD = 16
PASS_LEAD = 18
STRIP_FIRST = 12
STRIP_STEP = 3
OWNED = 4
OWNED_SMALL = 2
COARSE = 6
TILE = 32
STRIP_EARLY = 2
PLACE_PIECES = 4


def owned_by_half(zc, s_chunks):
    return min(OWNED if s_chunks > COARSE else OWNED_SMALL, zc // 4)


def drain(ref, sem):
    pltpu.make_async_copy(ref, ref, sem).wait()


def local(src, dst, sem):
    pltpu.make_async_copy(src, dst, sem).start()


def split(x):
    high = x.astype(jnp.bfloat16)
    low = (x - high.astype(jnp.float32)).astype(jnp.bfloat16)
    return high, low


def kernel(
    nr, nc, blk, s_chunks, r_first, zc, sc,
    start, deflated, z, s, r, f,
    zo, so, ro,
    fbuf, rot, rw, tw, acc, pair, xs,
    xb, xq, rv, rp, rr, rb, rq,
    load, f_far_send, f_own_recv, f_far_recv,
    f_row_send, f_row_recv, f_pass_send, f_pass_recv,
    x_send, x_own, x_far, o_send, o_recv, o_own, keep,
    r_in_send, r_in_recv, r_out_send, r_out_recv, r_own,
):
    row = lax.axis_index("row")
    col = lax.axis_index("col")
    tall, wide = f.shape
    width = nc * wide
    rows_per_chunk = z.shape[1]
    chunk_rounds = rows_per_chunk // blk
    chunks = zc + s_chunks
    crounds = r.shape[0] // tall
    lanes = r.shape[1]
    r_groups = crounds // nr
    half = nc // 2
    upper = col >= half
    base = jnp.where(upper, half, 0)
    far_base = half - base
    mid = jnp.where(upper, half, half - 1)
    far_mid = nc - 1 - mid
    mid_slot = jnp.where(upper, 0, half - 1)
    outer_base = jnp.where(upper, half + 1, 0)
    is_mid = col == mid
    sibling = row + 1 - 2 * lax.rem(row, 2)
    cores = nr // 2

    def send(src, dst, send_sem, recv_sem, target):
        pltpu.make_async_remote_copy(
            src_ref=src, dst_ref=dst, send_sem=send_sem, recv_sem=recv_sem,
            device_id=target, device_id_type=MESH,
        ).start()

    def row_peer(d):
        return lax.rem(row + d, nr)

    def half_peer(d):
        return base + lax.rem(col - base + d, half)

    local(f, fbuf.at[row, col], load.at[0])
    local(z, xb.at[pl.ds(0, zc), col], load.at[1])
    local(s, xb.at[pl.ds(zc, sc), col], load.at[2])
    local(r, rv, load.at[3])

    barrier = pltpu.get_barrier_semaphore()

    @pl.loop(1, nc)
    def _(d):
        pl.semaphore_signal(
            barrier, inc=1, device_id={"col": lax.rem(col + d, nc)}, device_id_type=MESH
        )

    @pl.loop(1, nr)
    def _(d):
        pl.semaphore_signal(barrier, inc=1, device_id={"row": row_peer(d)}, device_id_type=MESH)

    pl.semaphore_wait(barrier, nc + nr - 2)

    owned = owned_by_half(zc, s_chunks)
    side = upper.astype(jnp.int32)

    def mine(k):
        return (k < 2 * owned) & (lax.rem(k, 2) == side)

    def theirs(k):
        return (k < 2 * owned) & (lax.rem(k, 2) != side)

    def own_chunk(k):
        @pl.when(is_mid & jnp.logical_not(mine(k)))
        def _():
            send(xb.at[k, col], xb.at[k, col], x_send, x_far.at[k], {"col": far_mid})

        @pl.when(jnp.logical_not(is_mid))
        def _():
            send(xb.at[k, col], xb.at[k, col], x_send, x_own.at[k], {"col": mid})

    def pass_chunk(k):
        if half > 1:
            outers = pl.ds(outer_base, half - 1)
            drain(xb.at[k, pl.ds(0, half - 1)], x_own.at[k])

            @pl.when(jnp.logical_not(mine(k)))
            def _():
                send(xb.at[k, outers], xb.at[k, outers], x_send, x_far.at[k], {"col": far_mid})

    drain(fbuf.at[0, 0], load.at[0])

    @pl.when(is_mid)
    def _():
        send(fbuf.at[row, col], fbuf.at[row, col], f_far_send, f_far_recv, {"col": far_mid})

    for d in range(1, half):
        send(
            fbuf.at[row, col], fbuf.at[row, col], f_far_send, f_own_recv,
            {"col": half_peer(d)},
        )

    drain(xb.at[pl.ds(0, zc), 0], load.at[1])
    drain(xb.at[pl.ds(0, sc), 0], load.at[2])
    own_early = min(OWN_EARLY, chunks)
    own_first = min(max(OWN_LEAD, own_early), chunks)

    @pl.loop(0, jnp.where(is_mid, own_early, chunks))
    def _(k):
        own_chunk(k)

    drain(rv, load.at[3])
    if r_first < r_groups:
        @pl.loop(r_first * nr, crounds)
        def _(k):
            @pl.loop(0, tall // TILE)
            def _(i):
                first = pl.multiple_of(i * TILE, TILE)
                rp[k, pl.ds(first, TILE), :] = rv[
                    pl.ds(k + first * crounds, TILE, stride=crounds), :
                ]

    def r_in(first, last):
        if r_first < r_groups:
            @pl.loop(first, last)
            def _(g):
                @pl.loop(1, nr)
                def _(d):
                    p = row_peer(d)
                    send(rp.at[g * nr + p], rb.at[g, row], r_in_send, r_in_recv.at[g], {"row": p})

    strip_early = min(r_first + STRIP_EARLY, r_groups)
    strip_split = jnp.where(is_mid, r_first, strip_early)
    r_in(r_first, strip_split)

    if half > 1:
        drain(fbuf.at[0, pl.ds(0, half - 1)], f_own_recv)

        @pl.when(is_mid)
        def _():
            outers = pl.ds(outer_base, half - 1)
            send(
                fbuf.at[row, outers], fbuf.at[row, outers], f_far_send, f_far_recv,
                {"col": far_mid},
            )

    @pl.when(is_mid)
    def _():
        @pl.loop(own_early, own_first)
        def _(k):
            own_chunk(k)

    drain(fbuf.at[0, pl.ds(0, half)], f_far_recv)

    @pl.when(is_mid)
    def _():
        fars = pl.ds(far_base, half)
        for d in range(1, half):
            send(
                fbuf.at[row, fars], fbuf.at[row, fars], f_far_send, f_far_recv,
                {"col": half_peer(d)},
            )

    send(fbuf.at[row], fbuf.at[row], f_row_send, f_pass_recv.at[0], {"row": sibling})

    @pl.loop(1, cores)
    def _(d):
        send(fbuf.at[row], fbuf.at[row], f_row_send, f_row_recv.at[d], {"row": row_peer(2 * d)})

    pass_first = min(PASS_LEAD, chunks)

    r_in(strip_split, r_groups)

    @pl.when(is_mid)
    def _():
        @pl.loop(0, pass_first)
        def _(k):
            pass_chunk(k)

            @pl.when(k + own_first < chunks)
            def _():
                own_chunk(k + own_first)

    @pl.loop(1, cores)
    def _(d):
        drain(fbuf.at[0], f_row_recv.at[d])
        origin = row_peer(nr - 2 * d)
        send(fbuf.at[origin], fbuf.at[origin], f_pass_send, f_pass_recv.at[d], {"row": sibling})

    @pl.loop(0, cores)
    def _(d):
        drain(fbuf.at[0], f_pass_recv.at[d])

    kept = width - deflated[0]
    squares = jnp.zeros((1, 1), jnp.float32)
    spikes = []
    for c in range(nc):
        lane = lax.broadcasted_iota(jnp.int32, (1, wide), 1) + c * wide
        part = jnp.where(lane < kept, fbuf[0, c, 0:1, :], 0.0)
        squares = squares + jnp.sum(part * part, axis=1, keepdims=True)
        spikes.append((lane, part))
    corner = fbuf[0, 0, 0:1, 0:1]
    magnitude = jnp.sqrt(squares + 1e-06)
    shift = jnp.where(corner >= 0, 1.0, -1.0) * magnitude
    scaling = 2.0 / (squares + 2.0 * jnp.abs(corner) * magnitude + magnitude * magnitude)
    vector = [part + jnp.where(lane == 0, shift, 0.0) for lane, part in spikes]

    tiles = tall // TILE

    @pl.loop(0, nr * tiles)
    def _(t):
        i = t // tiles
        inner = pl.ds(pl.multiple_of(lax.rem(t, tiles) * TILE, TILE), TILE)
        rows = pl.ds(pl.multiple_of(t * TILE, TILE), TILE)
        image = fbuf[i, 0, inner, :] * vector[0]
        for c in range(1, nc):
            image = image + fbuf[i, c, inner, :] * vector[c]
        image = jnp.sum(image, axis=1, keepdims=True) * scaling
        for c in range(nc):
            rot[c, rows, :] = fbuf[i, c, inner, :] - image * vector[c]

    @pl.when(is_mid)
    def _():
        @pl.loop(0, nr * tiles)
        def _(t):
            rows = pl.ds(pl.multiple_of(t * TILE, TILE), TILE)

            @pl.loop(0, nc)
            def _(j):
                high, low = split(rot[lax.rem(base + j, nc), rows, :])
                rw[2 * j, rows, :] = high
                rw[2 * j + 1, rows, :] = low

    if r_first < r_groups:
        @pl.loop(0, width // 128)
        def _(i):
            rows = pl.ds(pl.multiple_of(i * 128, 128), 128)

            @pl.loop(0, nc)
            def _(c):
                high, low = split(rot[c, rows, :].T)
                per = wide // tall
                for q in range(per):
                    piece = slice(q * tall, (q + 1) * tall)
                    tw[c * per + q, :tall, rows] = high[piece]
                    tw[c * per + q, tall:, rows] = low[piece]

        def r_back(g):
            @pl.loop(1, nr)
            def _(d):
                p = row_peer(d)
                send(
                    rq.at[g, p], rr.at[g * nr + row], r_out_send, r_out_recv, {"row": p}
                )

        def r_group(g):
            rb[g, row] = rp[g * nr + row]
            drain(rb.at[g, pl.ds(0, nr - 1)], r_in_recv.at[g])

            @pl.loop(0, nr)
            def _(q):
                rows = pl.ds(pl.multiple_of(q * tall, tall), tall)
                high, low = split(rb[g, q])
                pair[rows, :lanes] = high
                pair[rows, lanes:] = low

            lane = lax.broadcasted_iota(jnp.int32, (1, lanes), 1)
            column = ((g * nr + row) * nc + col) * lanes + lane
            turned = column >= start[0] + width

            @pl.loop(0, nr)
            def _(q):
                both = jnp.dot(tw[q], pair[...], preferred_element_type=jnp.float32)
                both = both[:tall] + both[tall:]
                total = both[:, :lanes] + both[:, lanes:]
                rq[g, q] = jnp.where(turned, total, rb[g, q])

            rr[g * nr + row] = rq[g, row]

        def r_place():
            drain(rr.at[pl.ds(0, (r_groups - r_first) * (nr - 1))], r_out_recv)

            @pl.loop(r_first * nr, crounds)
            def _(k):
                @pl.loop(0, tall // TILE)
                def _(i):
                    first = pl.multiple_of(i * TILE, TILE)
                    rv[pl.ds(k + first * crounds, TILE, stride=crounds), :] = rr[
                        k, pl.ds(first, TILE), :
                    ]

            local(rv, ro, r_own)

    if s_chunks < sc:
        local(
            xb.at[pl.ds(zc + s_chunks, sc - s_chunks), col],
            so.at[pl.ds(s_chunks, sc - s_chunks)], keep,
        )

    def give(k):
        def to(out, n):
            local(xq.at[k * half + mid_slot], out.at[n], o_own)
            for d in range(1, half):
                j = lax.rem(mid_slot + d, half)
                send(xq.at[k * half + j], out.at[n], o_send, o_recv, {"col": base + j})

        @pl.when((k < zc) & jnp.logical_not(theirs(k)))
        def _():
            to(zo, k)

        if s_chunks:
            @pl.when(k >= zc)
            def _():
                to(so, k - zc)

    def give_far():
        @pl.loop(0, owned)
        def _(n):
            @pl.loop(0, half)
            def _(j):
                send(
                    xq.at[(chunks + n) * half + j], zo.at[2 * n + side], o_send, o_recv,
                    {"col": far_base + j},
                )

    strip_groups = r_groups - r_first
    strip_span = STRIP_STEP * strip_groups
    strip_first = min(STRIP_FIRST, chunks - strip_span - 4)

    @pl.loop(0, chunks)
    def _(k):
        @pl.when(is_mid)
        def _():
            @pl.when(k + pass_first < chunks)
            def _():
                pass_chunk(k + pass_first)

            @pl.when(k + pass_first + own_first < chunks)
            def _():
                own_chunk(k + pass_first + own_first)

            @pl.when(k > 0)
            def _():
                give(k - 1)

            @pl.when(k == max(chunks - pass_first, 2 * owned + 1))
            def _():
                give_far()

        if strip_groups > 0:
            step = k - strip_first
            g = r_first + step // STRIP_STEP
            active = (step >= 0) & (step < strip_span)

            @pl.when(active & (lax.rem(step, STRIP_STEP) == 0))
            def _():
                r_group(g)

            @pl.when(active & (lax.rem(step, STRIP_STEP) == 1))
            def _():
                r_back(g)

            @pl.when(k == chunks - 4)
            def _():
                r_place()

        @pl.when(is_mid & jnp.logical_not(theirs(k)))
        def _():
            drain(xb.at[k, pl.ds(0, half)], x_far.at[k])

            @pl.loop(0, nc)
            def _(c):
                columns = pl.ds(pl.multiple_of(c * wide, wide), wide)
                high, low = split(xb[k, c])
                xs[:rows_per_chunk, columns] = high
                xs[rows_per_chunk:, columns] = low

            index = lax.broadcasted_iota(jnp.int32, (rows_per_chunk, 1), 0)
            first = (k - zc) * chunk_rounds
            number = ((first + index // blk) * nr + row) * blk + lax.rem(index, blk)
            turned = number < jnp.where(k < zc, 2**30, start[0])

            @pl.loop(0, jnp.where(mine(k), 2 * nc, 2 * half))
            def _(i):
                both = jnp.dot(xs[...], rw[i], preferred_element_type=jnp.float32)
                both = both[:rows_per_chunk] + both[rows_per_chunk:]

                @pl.when(lax.rem(i, 2) == 0)
                def _():
                    acc[...] = both

                @pl.when(lax.rem(i, 2) == 1)
                def _():
                    j = i // 2
                    slot = jnp.where(j < half, k, chunks + k // 2 - 1) * half + j
                    xq[slot] = jnp.where(
                        turned, acc[...] + both, xb[k, lax.rem(base + j, nc)]
                    )

    @pl.when(is_mid)
    def _():
        give(chunks - 1)

    if strip_groups > 0:
        part = strip_groups * (nr - 1)
        drain(rr.at[pl.ds(0, part)], r_out_send)
        drain(rr.at[pl.ds(0, part)], r_in_send)
    else:
        local(rv, ro, r_own)
    drain(fbuf.at[pl.ds(0, cores)], f_row_send)
    if cores > 1:
        drain(fbuf.at[pl.ds(0, cores - 1)], f_pass_send)
    if half > 1:
        drain(fbuf.at[0, pl.ds(0, half - 1)], f_far_send)

    @pl.when(is_mid)
    def _():
        drain(fbuf.at[0, pl.ds(0, half)], f_far_send)
        for d in range(1, half):
            drain(fbuf.at[0, pl.ds(0, half)], f_far_send)
        drain(xb.at[pl.ds(0, chunks - owned), pl.ds(0, half)], x_send)
        drain(xq.at[pl.ds(0, (chunks - owned) * (half - 1) + owned * half)], o_send)
        drain(xq.at[pl.ds(0, chunks - owned)], o_own)
        if owned:
            drain(xq.at[pl.ds(0, owned)], o_recv)

    @pl.when(jnp.logical_not(is_mid))
    def _():
        drain(xb.at[pl.ds(0, chunks), 0], x_send)
        drain(xq.at[pl.ds(0, chunks)], o_recv)

    if s_chunks < sc:
        drain(so.at[pl.ds(s_chunks, sc - s_chunks)], keep)
    drain(rv, r_own)


def rotate(nr, nc, blk, s_chunks, r_first, ident, z, s, r, f, start, deflated):
    zc, rows_per_chunk, wide = z.shape
    sc = s.shape[0]
    tall = f.shape[0]
    width = nc * wide
    crounds = r.shape[0] // tall
    lanes = r.shape[1]
    r_groups = crounds // nr
    half = nc // 2
    chunks = zc + s_chunks
    smem = pl.BlockSpec(memory_space=pltpu.SMEM)
    hbm = pl.BlockSpec(memory_space=pltpu.HBM)
    f32 = jnp.float32
    bf16 = jnp.bfloat16
    dma = pltpu.SemaphoreType.DMA
    return pl.pallas_call(
        functools.partial(kernel, nr, nc, blk, s_chunks, r_first, zc, sc),
        out_shape=[jax.ShapeDtypeStruct(x.shape, f32) for x in (z, s, r)],
        in_specs=[smem] * 2 + [hbm] * 4,
        out_specs=[hbm] * 3,
        scratch_shapes=[
            pltpu.VMEM((nr, nc) + f.shape, f32),
            pltpu.VMEM((nc, width, wide), f32),
            pltpu.VMEM((2 * nc, width, wide), bf16),
            pltpu.VMEM((nr, 2 * tall, width), bf16),
            pltpu.VMEM((rows_per_chunk, wide), f32),
            pltpu.VMEM((width, 2 * lanes), bf16),
            pltpu.VMEM((2 * rows_per_chunk, width), bf16),
            pltpu.VMEM((zc + sc, nc, rows_per_chunk, wide), f32),
            pltpu.VMEM(((chunks + owned_by_half(zc, s_chunks)) * half, rows_per_chunk, wide), f32),
            pltpu.VMEM(r.shape, f32),
            pltpu.VMEM((crounds, tall, lanes), f32),
            pltpu.VMEM((crounds, tall, lanes), f32),
            pltpu.VMEM((r_groups, nr, tall, lanes), f32),
            pltpu.VMEM((r_groups, nr, tall, lanes), f32),
            dma((4,)), dma, dma, dma,
            dma, dma((nr // 2,)), dma, dma((nr // 2,)),
            dma, dma((chunks,)), dma((chunks,)), dma, dma, dma, dma,
            dma, dma((r_groups,)), dma, dma, dma,
        ],
        compiler_params=pltpu.CompilerParams(
            collective_id=ident, has_side_effects=True, vmem_limit_bytes=56 * 1024 * 1024,
        ),
    )(start, deflated, z, s, r, f)


def place(z, s, r, zo, so, ro, sb, rb, out, inn):
    step = z.shape[0] // PLACE_PIECES
    for j in range(PLACE_PIECES):
        rows = pl.ds(j * step, step)
        local(s.at[rows], sb.at[rows], inn.at[0, j])
    strip_step = r.shape[0] // PLACE_PIECES
    for j in range(PLACE_PIECES):
        rows = pl.ds(j * strip_step, strip_step)
        local(r.at[rows], rb.at[rows], inn.at[1, j])
    local(z, zo, out.at[0])
    for i, size, src, dst in ((0, step, sb, so), (1, strip_step, rb, ro)):
        for j in range(PLACE_PIECES):
            rows = pl.ds(j * size, size)
            drain(src.at[rows], inn.at[i, j])
            local(src.at[rows], dst.at[rows], out.at[1 + i])
    drain(z, out.at[0])
    drain(sb, out.at[1])
    drain(rb, out.at[2])


def placed(z, s, r):
    hbm = pl.BlockSpec(memory_space=pltpu.HBM)
    return pl.pallas_call(
        place,
        out_shape=[jax.ShapeDtypeStruct(x.shape, x.dtype) for x in (z, s, r)],
        in_specs=[pl.BlockSpec(memory_space=pltpu.VMEM), hbm, hbm],
        out_specs=[hbm] * 3,
        scratch_shapes=[
            pltpu.VMEM(s.shape, s.dtype),
            pltpu.VMEM(r.shape, r.dtype),
            pltpu.SemaphoreType.DMA((3,)),
            pltpu.SemaphoreType.DMA((2, PLACE_PIECES)),
        ],
        compiler_params=pltpu.CompilerParams(vmem_limit_bytes=8 * 1024 * 1024),
    )(z, s, r)


def body(vectors_window, column_strip, row_strip, factor, window_start, deflated):
    nr = lax.axis_size("row")
    nc = lax.axis_size("col")
    rounds, _, blk, wide = vectors_window.shape
    tall, column_rounds, _, lanes = row_strip.shape
    width = nc * wide
    per = ROUNDS_PER_CHUNK
    z = vectors_window.reshape(rounds // per, per * blk, wide)
    s = column_strip.reshape(rounds // per, per * blk, wide)
    r = row_strip.reshape(tall * column_rounds, lanes)
    chunk_rows = per * blk * nr
    group_columns = lanes * nr * nc
    count = -(-(rounds * nr * blk - width) // chunk_rows)
    coarse = COARSE if count > COARSE else 0
    sizes = [k for k in range(1, count + 1) if k > coarse or k % 2 == 0]
    bounds = [0] + sizes[:-1]
    branches = [
        functools.partial(
            rotate, nr, nc, blk, k, (low * chunk_rows + 1 + width) // group_columns, i
        )
        for i, (k, low) in enumerate(zip(sizes, bounds))
    ]
    last = jnp.clip((window_start[0] - 1) // chunk_rows, 0, count - 1)
    choice = jnp.where(last < coarse, last // 2, last - coarse // 2)
    zo, so, ro = lax.switch(choice, branches, z, s, r, factor, window_start, deflated)
    zo, so, ro = placed(zo, so, ro)
    return (
        zo.reshape(vectors_window.shape),
        so.reshape(column_strip.shape),
        ro.reshape(row_strip.shape),
    )


def solution(mesh):
    return jax.shard_map(
        body,
        mesh=mesh,
        in_specs=(
            P(None, "row", None, "col"),
            P(None, "row", None, "col"),
            P("row", None, "col", None),
            P("row", "col"),
            P(),
            P(),
        ),
        out_specs=(
            P(None, "row", None, "col"),
            P(None, "row", None, "col"),
            P("row", None, "col", None),
        ),
        check_vma=False,
    )
```
